32 devices in a mesh: dp: 8 (over z, x), cand: 4 (over y, core).
Axes of the slice: x: 2, y: 2, z: 4, core: 2. Of those that a mesh axis runs over, the one named last changes fastest.
Arguments:
- hidden: bfloat16 [16, 32, 128, 768], P('dp', 'cand'), may hold values from -24 to 24
- attn_weight: bfloat16 [768, 3072], P('dp'), may hold values from -1 to 1
- norm_gain: float32 [768], replicated, may hold values from 0.2 to 4
- pos_bias: float32 [12, 128, 128], replicated, may hold values from -5 to 5
- score_weight: float32 [768], replicated, may hold values from -4 to 4
- pair_lengths: int32 [16, 32], P('dp', 'cand'), may hold values from 32 to 128
- labels: int32 [16, 32], P('dp', 'cand'), may hold values from 0 to 3
Outputs:
- update: float32 [768, 3072], P('dp')
- loss: float32 [16], P('dp')
The draws below stay inside these ranges and needn't reach their ends.
All inputs are finite; a program needn't handle non-finite values.
Results may differ from the reference program's by a relative error of at most 0.017.
Values may be sent and summed in bfloat16 or wider, within the bound.
A program may use at most 128 MiB of HBM per device.

```python
import jax
import jax.numpy as jnp
from jax import lax

D = 768
HEADS = 12
HEAD = 64
SEQ = 128
CANDS = 32
QUERIES = 16


def draw_norm_gain(key, part):
    place = jnp.arange(D, dtype=jnp.int32).astype(jnp.float32) / jnp.float32(D)
    jitter = jax.random.uniform(jax.random.fold_in(key, 7401), (D,), jnp.float32, 0.75, 1.25)
    lowest, highest = (0.4, 2.0)
    values = jnp.exp(jnp.log(lowest) + (jnp.log(highest) - jnp.log(lowest)) * place) * jitter
    return jnp.clip(values, 0.2, 4.0)


def draw_score_weight(key, part):
    values = jax.random.normal(jax.random.fold_in(key, 7102), (D,), jnp.float32)
    values = jnp.clip(values, -6.0, 6.0) * jnp.sqrt(4.0 / jnp.float32(D))
    return jnp.clip(values, -4.0, 4.0)


def draw_attn_weight(key, part):
    values = jax.random.normal(jax.random.fold_in(key, 7301), (D, 4 * D), jnp.float32)
    values = jnp.clip(values, -6.0, 6.0) / jnp.sqrt(jnp.float32(D))
    column = jnp.arange(4 * D, dtype=jnp.int32)
    factor = jnp.where(column < D, 1.0 / jnp.sqrt(jnp.float32(HEAD)), 1.0)
    values = jnp.clip(values * factor[None, :], -1.0, 1.0)
    return values.astype(jnp.bfloat16)


def draw_hidden(key, part):
    normal_part = jax.random.normal(jax.random.fold_in(key, 7201), (QUERIES, CANDS, SEQ, D), jnp.float32)
    normal_part = jnp.clip(normal_part, -6.0, 6.0)
    values = normal_part
    return jnp.clip(values, -24.0, 24.0).astype(jnp.bfloat16)


def touch_ends(drawn, rng, least, largest):
    extent = drawn.shape
    index_at = [jax.random.randint(jax.random.fold_in(rng, axis), (), 0, extent[axis]) for axis in range(len(extent))]
    drawn = drawn.at[tuple(index_at)].set(least)
    longest = extent.index(max(extent))
    index_at[longest] = (index_at[longest] + 1) % extent[longest]
    return drawn.at[tuple(index_at)].set(largest)


def gaussian(stream_key, dims, scale, bound, kind=jnp.bfloat16):
    entries = jax.random.normal(stream_key, dims, jnp.float32) * scale
    return jnp.minimum(jnp.maximum(entries, -bound), bound).astype(kind)


def setup_inputs(seed: int = 0) -> dict:
    key_list = jax.random.split(jax.random.key(seed), 8)
    return {
        "hidden": draw_hidden(jax.random.fold_in(key_list[7], 71), 0),
        "attn_weight": draw_attn_weight(jax.random.fold_in(key_list[7], 71), 0),
        "norm_gain": draw_norm_gain(jax.random.fold_in(key_list[7], 71), 0),
        "pos_bias": gaussian(key_list[3], (HEADS, SEQ, SEQ), 1.0, 5.0, jnp.float32),
        "score_weight": draw_score_weight(jax.random.fold_in(key_list[7], 71), 0),
        "pair_lengths": touch_ends(jax.random.randint(key_list[5], (QUERIES, CANDS), SEQ // 4, SEQ + 1), jax.random.fold_in(key_list[5], 1), SEQ // 4, SEQ).astype(jnp.int32),
        "labels": touch_ends(jax.random.randint(key_list[6], (QUERIES, CANDS), 0, 4), jax.random.fold_in(key_list[6], 1), 0, 3).astype(jnp.int32),
    }


EPS = 1e-06

def rms_rows(values, gain):
    factor = lax.rsqrt(lax.optimization_barrier(jnp.mean(values * values, axis=-1, keepdims=True)) + EPS)
    return values * factor * gain

def attend(qkv, pos_bias, pair_len):
    batch, seq, triple = qkv.shape
    width = triple // 3
    heads = pos_bias.shape[0]
    head_size = width // heads
    parts = qkv.reshape(batch, seq, 3, heads, head_size).astype(jnp.float32)
    logits = jnp.einsum('bqhd,bkhd->bhqk', parts[:, :, 0], parts[:, :, 1])
    logits = logits + pos_bias[None]
    valid = jnp.arange(seq, dtype=jnp.int32)[None, :] < pair_len[:, None]
    logits = jnp.where(valid[:, None, None, :], logits, -1e+30)
    highest = lax.optimization_barrier(jnp.max(logits, axis=-1, keepdims=True))
    expo = jnp.exp(logits - highest)
    probs = (expo / lax.optimization_barrier(jnp.sum(expo, axis=-1, keepdims=True))).astype(jnp.bfloat16)
    context = jnp.einsum('bhqk,bkhd->bqhd', probs.astype(jnp.float32), parts[:, :, 2])
    return context.astype(jnp.bfloat16).reshape(batch, seq, width)

def forward(tokens, weights, norm_gain, pos_bias, pair_len):
    batch, seq, width = tokens.shape
    values = tokens.astype(jnp.float32)
    normed = rms_rows(values, norm_gain).astype(jnp.bfloat16)
    qkv = jnp.dot(normed.reshape(-1, width), weights[:, :3 * width], preferred_element_type=jnp.float32)
    qkv = qkv.astype(jnp.bfloat16).reshape(batch, seq, 3 * width)
    context = attend(qkv, pos_bias, pair_len)
    out_rows = values + jnp.dot(context.reshape(-1, width), weights[:, 3 * width:], preferred_element_type=jnp.float32).reshape(batch, seq, width)
    live = (jnp.arange(seq, dtype=jnp.int32)[None, :] < pair_len[:, None]).astype(jnp.float32)
    share = live / pair_len.astype(jnp.float32)[:, None]
    pooled = lax.optimization_barrier(jnp.sum(out_rows * share[:, :, None], axis=1))
    return (normed, qkv, context, pooled, share)

def score_head(pooled, score_weight):
    return lax.optimization_barrier(jnp.sum(rms_rows(pooled, 1.0) * score_weight, axis=-1))

def backward(normed, qkv, context, pooled, share, weights, pos_bias, pair_len, score_weight, score_grad):
    batch, seq, width = normed.shape
    unused, head_back = jax.vjp(lambda vector: score_head(vector, score_weight), pooled)
    pooled_grad = head_back(score_grad)[0]
    out_grad = (pooled_grad[:, None, :] * share[:, :, None]).astype(jnp.bfloat16)
    flat_out = out_grad.reshape(-1, width)
    context_grad = jnp.dot(flat_out, weights[:, 3 * width:].T, preferred_element_type=jnp.float32)
    context_grad = context_grad.astype(jnp.bfloat16).reshape(batch, seq, width)
    unused2, attend_back = jax.vjp(lambda block: attend(block, pos_bias, pair_len), qkv)
    qkv_grad = attend_back(context_grad)[0].reshape(-1, 3 * width)
    first = jnp.dot(normed.reshape(-1, width).T, qkv_grad, preferred_element_type=jnp.float32)
    second = jnp.dot(context.reshape(-1, width).T, flat_out, preferred_element_type=jnp.float32)
    return jnp.concatenate([first, second], axis=1)

def reference(hidden, attn_weight, norm_gain, pos_bias, score_weight, pair_lengths, labels):
    width = hidden.shape[3]

    def scores_of(pair):
        tokens, pair_len = pair
        unused_a, unused_b, unused_c, pooled, unused_d = forward(tokens, attn_weight, norm_gain, pos_bias, pair_len)
        return score_head(pooled, score_weight)
    scores = lax.map(scores_of, (hidden, pair_lengths))
    highest = lax.optimization_barrier(jnp.max(scores, axis=1, keepdims=True))
    expsum = lax.optimization_barrier(jnp.sum(jnp.exp(scores - highest), axis=1, keepdims=True))
    target = jnp.exp(labels.astype(jnp.float32))
    target_sum = lax.optimization_barrier(jnp.sum(target, axis=1, keepdims=True))
    target_dot = lax.optimization_barrier(jnp.sum(target * scores, axis=1, keepdims=True))
    loss = (highest + jnp.log(expsum) - target_dot / target_sum)[:, 0]
    score_grad = jnp.exp(scores - highest) / expsum - target / target_sum

    def accumulate(total, pair):
        tokens, pair_len, grad_row = pair
        normed, qkv, context, pooled, share = forward(tokens, attn_weight, norm_gain, pos_bias, pair_len)
        term = backward(normed, qkv, context, pooled, share, attn_weight, pos_bias, pair_len, score_weight, grad_row)
        return (total + term, None)
    start = jnp.zeros((width, 4 * width), jnp.float32)
    grad, unused = lax.scan(accumulate, start, (hidden, pair_lengths, score_grad))
    rms_value = jnp.sqrt(jnp.sum(grad * grad) / (4.0 * width * width))
    update = grad / (rms_value + EPS)
    return (update, loss)
```

```python
import functools

import jax
import jax.numpy as jnp
from jax import lax
from jax.experimental import pallas as pl
from jax.experimental.pallas import tpu as pltpu
from jax.sharding import PartitionSpec as P

EPS = 1e-06
F32 = jnp.float32
BF16 = jnp.bfloat16
VMEM_LIMIT = 60 * 1024 * 1024
NT = (((1,), (1,)), ((), ()))
TN = (((0,), (0,)), ((), ()))


def half_masks(lanes):
    lane = lax.broadcasted_iota(jnp.int32, (1, lanes), 1)
    low = (lane < lanes // 2).astype(F32)
    return low.astype(BF16), (1.0 - low).astype(BF16)


def stack_halves(block, low, high):
    return jnp.concatenate([block * low, block * high], axis=0)


def forward_kernel(hpad, len_ref, h_ref, gain_ref, w_ref, bias_ref, nt_ref, qk_ref, p_ref, u_ref, hsum_ref, norm_scr):
    batch, seq, width = h_ref.shape
    heads = bias_ref.shape[0]
    duo = 2 * (width // heads)
    step = pl.program_id(0)
    values = h_ref[...].reshape(batch * seq, width).astype(F32)
    factor = lax.rsqrt(jnp.mean(values * values, axis=-1, keepdims=True) + EPS)
    normed = (values * factor * gain_ref[...]).astype(BF16)
    norm_scr[...] = normed.reshape(batch, seq, width)
    nt_ref[...] = normed.T
    qk = jnp.dot(normed, w_ref[...], preferred_element_type=F32)
    qk_ref[...] = qk.astype(BF16).reshape(batch, seq, 2 * width)
    low, high = half_masks(duo)
    col = lax.broadcasted_iota(jnp.int32, (1, seq), 1)
    row = lax.broadcasted_iota(jnp.int32, (seq, 1), 0)

    def pair(i, carry):
        length = len_ref[step * batch + i]
        penalty = jnp.where(col < length, 0.0, 1.0) > 0.5
        live = row < length
        live2 = jnp.concatenate([live.astype(F32)] * 2, axis=0)
        sums = []
        for hp in range(heads // 2):
            q2 = qk_ref[i, :, hp * duo : (hp + 1) * duo]
            k2 = qk_ref[i, :, width + hp * duo : width + (hp + 1) * duo]
            logits = lax.dot_general(stack_halves(q2, low, high), k2, NT, preferred_element_type=F32)
            logits = logits + bias_ref[2 * hp : 2 * hp + 2].reshape(2 * seq, seq)
            logits = jnp.where(penalty, -1e30, logits)
            expo = jnp.exp(logits - jnp.max(logits, axis=-1, keepdims=True))
            inv = live2 / jnp.sum(expo, axis=-1, keepdims=True)
            probs = (expo * inv).astype(BF16)
            p_ref[i, 2 * hp : 2 * hp + 2] = probs.reshape(2, seq, seq)
            sums.append(jnp.sum(probs.astype(F32).reshape(2, seq, seq), axis=1))
        if hpad > heads:
            sums.append(jnp.zeros((hpad - heads, seq), F32))
        weights = jnp.concatenate(sums, axis=0).astype(BF16)
        u_ref[i] = jnp.dot(weights, norm_scr[i], preferred_element_type=F32).astype(BF16)
        rows = h_ref[i].astype(F32) * live.astype(F32)
        hsum_ref[i] = jnp.sum(rows, axis=0, keepdims=True)
        return carry

    lax.fori_loop(0, batch, pair, 0)


def forward(tokens, pair_len, gain, wqk, pos_bias):
    pairs, seq, width = tokens.shape
    heads = pos_bias.shape[0]
    hpad = -(-heads // 16) * 16
    batch = 4 if pairs % 4 == 0 else 1
    full = lambda *shape: pl.BlockSpec(shape, lambda i: (0,) * len(shape))
    return pl.pallas_call(
        functools.partial(forward_kernel, hpad),
        grid=(pairs // batch,),
        in_specs=[
            pl.BlockSpec(memory_space=pltpu.SMEM),
            pl.BlockSpec((batch, seq, width), lambda i: (i, 0, 0)),
            full(1, width),
            full(width, 2 * width),
            full(heads, seq, seq),
        ],
        out_specs=[
            pl.BlockSpec((width, batch * seq), lambda i: (0, i)),
            pl.BlockSpec((batch, seq, 2 * width), lambda i: (i, 0, 0)),
            pl.BlockSpec((batch, heads, seq, seq), lambda i: (i, 0, 0, 0)),
            pl.BlockSpec((batch, hpad, width), lambda i: (i, 0, 0)),
            pl.BlockSpec((batch, 1, width), lambda i: (i, 0, 0)),
        ],
        out_shape=[
            jax.ShapeDtypeStruct((width, pairs * seq), BF16),
            jax.ShapeDtypeStruct((pairs, seq, 2 * width), BF16),
            jax.ShapeDtypeStruct((pairs, heads, seq, seq), BF16),
            jax.ShapeDtypeStruct((pairs, hpad, width), BF16),
            jax.ShapeDtypeStruct((pairs, 1, width), F32),
        ],
        scratch_shapes=[pltpu.VMEM((batch, seq, width), BF16)],
        compiler_params=pltpu.CompilerParams(vmem_limit_bytes=VMEM_LIMIT),
        cost_estimate=pl.CostEstimate(flops=30_000_000_000, bytes_accessed=24_000_000, transcendentals=0),
        name="attend_forward",
    )(pair_len, tokens, gain, wqk, pos_bias)


def head_mask(hpad, width, head_size):
    lane = lax.broadcasted_iota(jnp.int32, (hpad, width), 1)
    head = lax.broadcasted_iota(jnp.int32, (hpad, width), 0)
    start = head * head_size
    return ((lane >= start) & (lane < start + head_size)).astype(F32)


def score_kernel(head_size, u_ref, wv_ref, wo_ref, hsum_ref, len_ref, sw_ref, ctx_ref, pooled_ref, score_ref):
    pairs, hpad, width = u_ref.shape
    mixed = jnp.dot(u_ref[...].reshape(pairs * hpad, width), wv_ref[...], preferred_element_type=F32)
    mask = head_mask(hpad, width, head_size)
    ctx = jnp.sum(mixed.reshape(pairs, hpad, width) * mask[None], axis=1)
    ctx_ref[...] = ctx.astype(BF16)
    share = 1.0 / len_ref[...]
    mean = ctx * share
    high = mean.astype(BF16)
    low = (mean - high.astype(F32)).astype(BF16)
    both = jnp.dot(jnp.concatenate([high, low], axis=0), wo_ref[...], preferred_element_type=F32)
    pooled = hsum_ref[...] * share + both[:pairs] + both[pairs:]
    pooled_ref[...] = pooled
    factor = lax.rsqrt(jnp.mean(pooled * pooled, axis=-1, keepdims=True) + EPS)
    score_ref[...] = jnp.sum(pooled * factor * sw_ref[...], axis=-1, keepdims=True)


def middle_kernel(head_size, sg_ref, pooled_ref, len_ref, sw_ref, u_ref, ctx_ref, wv_ref, wo_ref, wc_ref, gvo_ref):
    pairs, hpad, width = u_ref.shape
    pooled = pooled_ref[...]
    sw = sw_ref[...]
    factor = lax.rsqrt(jnp.mean(pooled * pooled, axis=-1, keepdims=True) + EPS)
    dot = jnp.sum(pooled * sw, axis=-1, keepdims=True) * (1.0 / width)
    grad = sg_ref[...] * (factor * sw - pooled * (factor * factor * factor * dot))
    out_grad = (grad / len_ref[...]).astype(BF16)
    cg = lax.dot_general(out_grad, wo_ref[...], NT, preferred_element_type=F32).astype(BF16).astype(F32)
    mask = head_mask(hpad, width, head_size)
    spread = (cg[:, None, :] * mask[None]).astype(BF16).reshape(pairs * hpad, width)
    wc = lax.dot_general(spread, wv_ref[...], NT, preferred_element_type=F32)
    wc_ref[...] = wc.astype(BF16).reshape(pairs, hpad, width)
    u = u_ref[...].reshape(pairs * hpad, width)
    gvo_ref[:, :width] = lax.dot_general(u, spread, TN, preferred_element_type=F32).astype(BF16)
    gvo_ref[:, width:] = lax.dot_general(ctx_ref[...], out_grad, TN, preferred_element_type=F32).astype(BF16)


def backward_kernel(nt_ref, q_ref, k_ref, p_ref, wc_ref, g_ref, dp_scr, dqk_scr):
    pairs, seq, duo = q_ref.shape
    heads2 = dp_scr.shape[0]
    hp = pl.program_id(0)

    @pl.when(hp == 0)
    def _():
        for i in range(pairs):
            rows = jnp.dot(wc_ref[i], nt_ref[:, i * seq : (i + 1) * seq], preferred_element_type=F32)
            for j in range(heads2):
                dp_scr[j, i] = rows[2 * j : 2 * j + 2]

    low, high = half_masks(duo)

    def pair(i, carry):
        probs = p_ref[i].astype(F32)
        term = probs * dp_scr[hp, i][:, None, :]
        dlog = (term - probs * jnp.sum(term, axis=-1, keepdims=True)).astype(BF16)
        wide = jnp.concatenate([dlog[0], dlog[1]], axis=1)
        dq = jnp.dot(wide, stack_halves(k_ref[i], low, high), preferred_element_type=F32)
        dk = lax.dot_general(
            dlog.reshape(2 * seq, seq), stack_halves(q_ref[i], low, high), TN, preferred_element_type=F32
        )
        dqk_scr[i, :, :duo] = dq.astype(BF16)
        dqk_scr[i, :, duo:] = dk.astype(BF16)
        return carry

    lax.fori_loop(0, pairs, pair, 0, unroll=4)
    grad = jnp.dot(nt_ref[...], dqk_scr[...].reshape(pairs * seq, 2 * duo), preferred_element_type=F32)
    g_ref[0] = grad[:, :duo].astype(BF16)
    g_ref[1] = grad[:, duo:].astype(BF16)


def backward(normed_t, qk, probs, wc):
    pairs, heads, seq, _ = probs.shape
    width = normed_t.shape[0]
    duo = 2 * (width // heads)
    duos = heads // 2
    return pl.pallas_call(
        backward_kernel,
        grid=(duos,),
        in_specs=[
            pl.BlockSpec((width, pairs * seq), lambda h: (0, 0)),
            pl.BlockSpec((pairs, seq, duo), lambda h: (0, 0, h)),
            pl.BlockSpec((pairs, seq, duo), lambda h: (0, 0, duos + h)),
            pl.BlockSpec((pairs, 2, seq, seq), lambda h: (0, h, 0, 0)),
            pl.BlockSpec(wc.shape, lambda h: (0, 0, 0)),
        ],
        out_specs=pl.BlockSpec((2, width, duo), lambda h: (0, 0, h)),
        out_shape=jax.ShapeDtypeStruct((2, width, width), BF16),
        scratch_shapes=[pltpu.VMEM((duos, pairs, 2, seq), F32), pltpu.VMEM((pairs, seq, 2 * duo), BF16)],
        compiler_params=pltpu.CompilerParams(vmem_limit_bytes=VMEM_LIMIT),
        cost_estimate=pl.CostEstimate(flops=30_000_000_000, bytes_accessed=20_000_000, transcendentals=0),
        name="attend_backward",
    )(normed_t, qk, qk, probs, wc)


def shards(hidden, attn_weight, norm_gain, pos_bias, score_weight, pair_lengths, labels):
    q_local, c_local, seq, width = hidden.shape
    pairs = q_local * c_local
    heads = pos_bias.shape[0]
    head_size = width // heads
    wqk = lax.all_gather(attn_weight[:, : 2 * width], "dp", axis=0, tiled=True)
    wvo = lax.all_gather(attn_weight[:, 2 * width :], "dp", axis=0, tiled=True)
    wv, wo = wvo[:, :width], wvo[:, width:]
    pair_len = pair_lengths.reshape(pairs)
    len_col = pair_len.astype(F32).reshape(pairs, 1)
    gain = norm_gain.reshape(1, width)
    sw = score_weight.reshape(1, width)
    tokens = hidden.reshape(pairs, seq, width)
    normed_t, qk, probs, u, hsum = forward(tokens, pair_len, gain, wqk, pos_bias)
    params = pltpu.CompilerParams(vmem_limit_bytes=VMEM_LIMIT)
    ctx, pooled, score_col = pl.pallas_call(
        functools.partial(score_kernel, head_size),
        out_shape=[
            jax.ShapeDtypeStruct((pairs, width), BF16),
            jax.ShapeDtypeStruct((pairs, width), F32),
            jax.ShapeDtypeStruct((pairs, 1), F32),
        ],
        compiler_params=params,
        name="score_forward",
    )(u, wv, wo, hsum.reshape(pairs, width), len_col, sw)
    scores = score_col.reshape(q_local, c_local)
    mine = jnp.stack([scores, labels.astype(F32)])
    every = lax.all_gather(mine, "cand", axis=2, tiled=True)
    all_scores, all_target = every[0], jnp.exp(every[1])
    highest = jnp.max(all_scores, axis=1)
    expsum = jnp.sum(jnp.exp(all_scores - highest[:, None]), axis=1)
    target_sum = jnp.sum(all_target, axis=1)
    target_dot = jnp.sum(all_target * all_scores, axis=1)
    loss = highest + jnp.log(expsum) - target_dot / target_sum
    target = jnp.exp(labels.astype(F32))
    score_grad = jnp.exp(scores - highest[:, None]) / expsum[:, None] - target / target_sum[:, None]
    wc, gvo = pl.pallas_call(
        functools.partial(middle_kernel, head_size),
        out_shape=[
            jax.ShapeDtypeStruct(u.shape, BF16),
            jax.ShapeDtypeStruct((width, 2 * width), BF16),
        ],
        compiler_params=params,
        name="score_backward",
    )(score_grad.reshape(pairs, 1), pooled, len_col, sw, u, ctx, wv, wo)
    gvo = lax.psum_scatter(gvo, "dp", scatter_dimension=0, tiled=True)
    gqk = backward(normed_t, qk, probs, wc)
    gqk = lax.psum_scatter(gqk, "dp", scatter_dimension=1, tiled=True)
    shard = jnp.concatenate([gqk[0], gqk[1], gvo], axis=1)
    shard = lax.psum(shard, "cand").astype(F32)
    squares = lax.psum(jnp.sum(shard * shard), "dp")
    rms_value = jnp.sqrt(squares / (4.0 * width * width))
    update = shard / (rms_value + EPS)
    return (update, loss)


def solution(mesh):
    in_specs = (
        P("dp", "cand", None, None),
        P("dp", None),
        P(),
        P(),
        P(),
        P("dp", "cand"),
        P("dp", "cand"),
    )
    out_specs = (P("dp", None), P("dp"))
    return jax.shard_map(shards, mesh=mesh, in_specs=in_specs, out_specs=out_specs, check_vma=False)
```

```python
import functools

import jax
import jax.numpy as jnp
from jax import lax
from jax.experimental import pallas as pl
from jax.experimental.pallas import tpu as pltpu
from jax.sharding import PartitionSpec as P

EPS = 1e-06
F32 = jnp.float32
BF16 = jnp.bfloat16
VMEM_LIMIT = 60 * 1024 * 1024
NT = (((1,), (1,)), ((), ()))
TN = (((0,), (0,)), ((), ()))


def half_masks(lanes):
    lane = lax.broadcasted_iota(jnp.int32, (1, lanes), 1)
    low = (lane < lanes // 2).astype(F32)
    return low.astype(BF16), (1.0 - low).astype(BF16)


def stack_halves(block, low, high):
    return jnp.concatenate([block * low, block * high], axis=0)


def forward_kernel(hpad, len_ref, h_ref, gain_ref, w_ref, bias_ref, nt_ref, qk_ref, p_ref, u_ref, hsum_ref, norm_scr):
    batch, seq, width = h_ref.shape
    heads = bias_ref.shape[0]
    duo = 2 * (width // heads)
    step = pl.program_id(0)
    values = h_ref[...].reshape(batch * seq, width).astype(F32)
    factor = lax.rsqrt(jnp.mean(values * values, axis=-1, keepdims=True) + EPS)
    normed = (values * factor * gain_ref[...]).astype(BF16)
    norm_scr[...] = normed.reshape(batch, seq, width)
    nt_ref[...] = normed.T
    for part in range(2):
        proj = jnp.dot(normed, w_ref[part], preferred_element_type=F32)
        qk_ref[:, :, part * width : (part + 1) * width] = proj.astype(BF16).reshape(batch, seq, width)
    low, high = half_masks(duo)
    col = lax.broadcasted_iota(jnp.int32, (1, seq), 1)
    row = lax.broadcasted_iota(jnp.int32, (seq, 1), 0)

    def pair(i, carry):
        length = len_ref[step * batch + i]
        penalty = jnp.where(col < length, 0.0, 1.0) > 0.5
        live = row < length
        live2 = jnp.concatenate([live.astype(F32)] * 2, axis=0)
        sums = []
        for hp in range(heads // 2):
            q2 = qk_ref[i, :, hp * duo : (hp + 1) * duo]
            k2 = qk_ref[i, :, width + hp * duo : width + (hp + 1) * duo]
            logits = lax.dot_general(stack_halves(q2, low, high), k2, NT, preferred_element_type=F32)
            logits = logits + bias_ref[2 * hp : 2 * hp + 2].reshape(2 * seq, seq)
            logits = jnp.where(penalty, -1e30, logits)
            expo = jnp.exp(logits - jnp.max(logits, axis=-1, keepdims=True))
            inv = live2 / jnp.sum(expo, axis=-1, keepdims=True)
            probs = (expo * inv).astype(BF16)
            p_ref[i, 2 * hp : 2 * hp + 2] = probs.reshape(2, seq, seq)
            sums.append(jnp.sum(probs.astype(F32).reshape(2, seq, seq), axis=1))
        if hpad > heads:
            sums.append(jnp.zeros((hpad - heads, seq), F32))
        weights = jnp.concatenate(sums, axis=0).astype(BF16)
        u_ref[i] = jnp.dot(weights, norm_scr[i], preferred_element_type=F32).astype(BF16)
        rows = h_ref[i].astype(F32) * live.astype(F32)
        hsum_ref[i] = jnp.sum(rows, axis=0, keepdims=True)
        return carry

    lax.fori_loop(0, batch, pair, 0)


def forward(tokens, pair_len, gain, weights, pos_bias):
    pairs, seq, width = tokens.shape
    heads = pos_bias.shape[0]
    hpad = -(-heads // 16) * 16
    batch = 4 if pairs % 4 == 0 else 1
    full = lambda *shape: pl.BlockSpec(shape, lambda i: (0,) * len(shape))
    return pl.pallas_call(
        functools.partial(forward_kernel, hpad),
        grid=(pairs // batch,),
        in_specs=[
            pl.BlockSpec(memory_space=pltpu.SMEM),
            pl.BlockSpec((batch, seq, width), lambda i: (i, 0, 0)),
            full(1, width),
            full(2, width, width),
            full(heads, seq, seq),
        ],
        out_specs=[
            pl.BlockSpec((width, batch * seq), lambda i: (0, i)),
            pl.BlockSpec((batch, seq, 2 * width), lambda i: (i, 0, 0)),
            pl.BlockSpec((batch, heads, seq, seq), lambda i: (i, 0, 0, 0)),
            pl.BlockSpec((batch, hpad, width), lambda i: (i, 0, 0)),
            pl.BlockSpec((batch, 1, width), lambda i: (i, 0, 0)),
        ],
        out_shape=[
            jax.ShapeDtypeStruct((width, pairs * seq), BF16),
            jax.ShapeDtypeStruct((pairs, seq, 2 * width), BF16),
            jax.ShapeDtypeStruct((pairs, heads, seq, seq), BF16),
            jax.ShapeDtypeStruct((pairs, hpad, width), BF16),
            jax.ShapeDtypeStruct((pairs, 1, width), F32),
        ],
        scratch_shapes=[pltpu.VMEM((batch, seq, width), BF16)],
        compiler_params=pltpu.CompilerParams(vmem_limit_bytes=VMEM_LIMIT),
        cost_estimate=pl.CostEstimate(flops=30_000_000_000, bytes_accessed=24_000_000, transcendentals=0),
        name="attend_forward",
    )(pair_len, tokens, gain, weights, pos_bias)


def head_mask(hpad, width, head_size):
    lane = lax.broadcasted_iota(jnp.int32, (hpad, width), 1)
    head = lax.broadcasted_iota(jnp.int32, (hpad, width), 0)
    start = head * head_size
    return ((lane >= start) & (lane < start + head_size)).astype(F32)


def score_kernel(head_size, u_ref, w_ref, hsum_ref, len_ref, sw_ref, ctx_ref, pooled_ref, score_ref):
    pairs, hpad, width = u_ref.shape
    mixed = jnp.dot(u_ref[...].reshape(pairs * hpad, width), w_ref[0], preferred_element_type=F32)
    mask = head_mask(hpad, width, head_size)
    ctx = jnp.sum(mixed.reshape(pairs, hpad, width) * mask[None], axis=1)
    ctx_ref[...] = ctx.astype(BF16)
    share = 1.0 / len_ref[...]
    mean = ctx * share
    high = mean.astype(BF16)
    low = (mean - high.astype(F32)).astype(BF16)
    both = jnp.dot(jnp.concatenate([high, low], axis=0), w_ref[1], preferred_element_type=F32)
    pooled = hsum_ref[...] * share + both[:pairs] + both[pairs:]
    pooled_ref[...] = pooled
    factor = lax.rsqrt(jnp.mean(pooled * pooled, axis=-1, keepdims=True) + EPS)
    score_ref[...] = jnp.sum(pooled * factor * sw_ref[...], axis=-1, keepdims=True)


def middle_kernel(head_size, sg_ref, pooled_ref, len_ref, sw_ref, u_ref, ctx_ref, w_ref, wc_ref, gvo_ref):
    pairs, hpad, width = u_ref.shape
    pooled = pooled_ref[...]
    sw = sw_ref[...]
    factor = lax.rsqrt(jnp.mean(pooled * pooled, axis=-1, keepdims=True) + EPS)
    dot = jnp.sum(pooled * sw, axis=-1, keepdims=True) * (1.0 / width)
    grad = sg_ref[...] * (factor * sw - pooled * (factor * factor * factor * dot))
    out_grad = (grad / len_ref[...]).astype(BF16)
    cg = lax.dot_general(out_grad, w_ref[1], NT, preferred_element_type=F32).astype(BF16).astype(F32)
    mask = head_mask(hpad, width, head_size)
    spread = (cg[:, None, :] * mask[None]).astype(BF16).reshape(pairs * hpad, width)
    wc = lax.dot_general(spread, w_ref[0], NT, preferred_element_type=F32)
    wc_ref[...] = wc.astype(BF16).reshape(pairs, hpad, width)
    u = u_ref[...].reshape(pairs * hpad, width)
    _, duos, _, lanes = gvo_ref.shape
    gv = lax.dot_general(u, spread, TN, preferred_element_type=F32).astype(BF16)
    go = lax.dot_general(ctx_ref[...], out_grad, TN, preferred_element_type=F32).astype(BF16)
    for j in range(duos):
        gvo_ref[0, j] = gv[:, j * lanes : (j + 1) * lanes]
        gvo_ref[1, j] = go[:, j * lanes : (j + 1) * lanes]


def backward_kernel(nt_ref, q_ref, k_ref, p_ref, wc_ref, gin_ref, g_ref, dp_scr, dqk_scr):
    pairs, seq, duo = q_ref.shape
    heads2 = dp_scr.shape[0]
    hp = pl.program_id(0)

    @pl.when(hp == 0)
    def _():
        for i in range(pairs):
            rows = jnp.dot(wc_ref[i], nt_ref[:, i * seq : (i + 1) * seq], preferred_element_type=F32)
            for j in range(heads2):
                dp_scr[j, i] = rows[2 * j : 2 * j + 2]

    low, high = half_masks(duo)

    def pair(i, carry):
        probs = p_ref[i].astype(F32)
        term = probs * dp_scr[hp, i][:, None, :]
        dlog = (term - probs * jnp.sum(term, axis=-1, keepdims=True)).astype(BF16)
        wide = jnp.concatenate([dlog[0], dlog[1]], axis=1)
        dq = jnp.dot(wide, stack_halves(k_ref[i], low, high), preferred_element_type=F32)
        dk = lax.dot_general(
            dlog.reshape(2 * seq, seq), stack_halves(q_ref[i], low, high), TN, preferred_element_type=F32
        )
        dqk_scr[i, :, :duo] = dq.astype(BF16)
        dqk_scr[i, :, duo:] = dk.astype(BF16)
        return carry

    lax.fori_loop(0, pairs, pair, 0, unroll=4)
    grad = jnp.dot(nt_ref[...], dqk_scr[...].reshape(pairs * seq, 2 * duo), preferred_element_type=F32)
    g_ref[0, 0] = grad[:, :duo].astype(BF16)
    g_ref[1, 0] = grad[:, duo:].astype(BF16)


def backward(normed_t, qk, probs, wc, grads):
    pairs, heads, seq, _ = probs.shape
    width = normed_t.shape[0]
    duo = 2 * (width // heads)
    duos = heads // 2
    return pl.pallas_call(
        backward_kernel,
        grid=(duos,),
        in_specs=[
            pl.BlockSpec((width, pairs * seq), lambda h: (0, 0)),
            pl.BlockSpec((pairs, seq, duo), lambda h: (0, 0, h)),
            pl.BlockSpec((pairs, seq, duo), lambda h: (0, 0, duos + h)),
            pl.BlockSpec((pairs, 2, seq, seq), lambda h: (0, h, 0, 0)),
            pl.BlockSpec(wc.shape, lambda h: (0, 0, 0)),
            pl.BlockSpec(memory_space=pl.ANY),
        ],
        out_specs=pl.BlockSpec((2, 1, width, duo), lambda h: (0, h, 0, 0)),
        out_shape=jax.ShapeDtypeStruct(grads.shape, BF16),
        input_output_aliases={5: 0},
        scratch_shapes=[pltpu.VMEM((duos, pairs, 2, seq), F32), pltpu.VMEM((pairs, seq, 2 * duo), BF16)],
        compiler_params=pltpu.CompilerParams(vmem_limit_bytes=VMEM_LIMIT),
        cost_estimate=pl.CostEstimate(flops=30_000_000_000, bytes_accessed=20_000_000, transcendentals=0),
        name="attend_backward",
    )(normed_t, qk, qk, probs, wc, grads)


MESH = pl.DeviceIdType.MESH


def greet(targets):
    barrier = pltpu.get_barrier_semaphore()
    for target in targets:
        pl.semaphore_signal(barrier, inc=1, device_id=target, device_id_type=MESH)
    pl.semaphore_wait(barrier, len(targets))


def push(src, dst, send, recv, target):
    copy = pltpu.make_async_remote_copy(
        src_ref=src, dst_ref=dst, send_sem=send, recv_sem=recv, device_id=target, device_id_type=MESH
    )
    copy.start()
    return copy


def gather_kernel(n, m, x_ref, o_ref, own_sem, z_send, x_send, y_send, c_send, recv):
    rows = x_ref.shape[0]
    wide = x_ref.shape[1] // m
    half, duo = n // 2, m // 2
    d, c = lax.axis_index("dp"), lax.axis_index("cand")
    z, x = d // 2, d % 2
    y, core = c // 2, c % 2
    across = (d + 1 - 2 * x, c)
    other = (d, c + 1 - 2 * core)
    zs = [(2 * lax.rem(z + j, half) + x, c) for j in range(1, half)]
    ys = [(d, 2 * lax.rem(y + j, duo) + core) for j in range(1, duo)]
    greet(zs + ys + [across, other])
    mine = x_ref.at[:, pl.ds(pl.multiple_of(c * wide, 128), wide)]
    copies = []
    for j in range(half - 1):
        copies.append(push(mine, o_ref.at[c, d], z_send.at[j], recv.at[c, d], zs[j]))
    copies.append(push(mine, o_ref.at[c, d], x_send.at[0], recv.at[c, d], across))
    local = []
    for k in range(m):
        local.append(
            pltpu.make_async_copy(x_ref.at[:, k * wide : (k + 1) * wide], o_ref.at[k, d], own_sem.at[k])
        )
        local[-1].start()

    def arrived(piece, block):
        ref = o_ref.at[piece, block]
        pltpu.make_async_copy(ref, ref, recv.at[piece, block]).wait()

    def spread(block, slot):
        ref = o_ref.at[c, block]
        for j in range(duo - 1):
            copies.append(push(ref, ref, y_send.at[slot, j], recv.at[c, block], ys[j]))
        copies.append(push(ref, ref, c_send.at[0, slot], recv.at[c, block], other))

    for j in range(1, half):
        block = 2 * lax.rem(z - j + half, half) + x
        arrived(c, block)
        ref = o_ref.at[c, block]
        copies.append(push(ref, ref, x_send.at[j], recv.at[c, block], across))
        spread(block, j - 1)
    far = []
    for j in range(half):
        block = 2 * lax.rem(z - j + half, half) + 1 - x
        arrived(c, block)
        spread(block, half - 1 + j)
    order = [2 * lax.rem(z - j + half, half) + x for j in range(1, half)]
    order += [2 * lax.rem(z - j + half, half) + 1 - x for j in range(half)]
    for slot, block in enumerate(order):
        for j in range(1, duo):
            piece = 2 * lax.rem(y - j + duo, duo) + core
            arrived(piece, block)
            ref = o_ref.at[piece, block]
            copies.append(push(ref, ref, c_send.at[j, slot], recv.at[piece, block], other))
    for slot, block in enumerate(order):
        for j in range(duo):
            arrived(2 * lax.rem(y - j + duo, duo) + 1 - core, block)
    for copy in local:
        copy.wait()
    for copy in copies:
        copy.wait_send()


def gather_weights(block, n, m):
    rows, total = block.shape
    dma = pltpu.SemaphoreType.DMA
    return pl.pallas_call(
        functools.partial(gather_kernel, n, m),
        in_specs=[pl.BlockSpec(memory_space=pltpu.VMEM)],
        out_specs=pl.BlockSpec(memory_space=pltpu.VMEM),
        out_shape=jax.ShapeDtypeStruct((m, n, rows, total // m), block.dtype),
        scratch_shapes=[
            dma((m,)), dma((n // 2,)), dma((n // 2,)), dma((n, max(m // 2 - 1, 1))), dma((m // 2, n)), dma((m, n))
        ],
        compiler_params=pltpu.CompilerParams(
            collective_id=0, has_side_effects=True, vmem_limit_bytes=VMEM_LIMIT
        ),
        name="gather_weights",
    )(block)


def reduce_kernel(n, m, g_ref, o_ref, r1, s1, r2, s2, r3, s3, r4, fin, sq, r6,
                  t1, v1, t2, v2, t3, v3, t4, v4, t5, v5, t6, v6):
    chunks, duo, _, half, _, rows, lanes = g_ref.shape
    d, c = lax.axis_index("dp"), lax.axis_index("cand")
    z, x = d // 2, d % 2
    y, core = c // 2, c % 2
    across = (d + 1 - 2 * x, c)
    other = (d, c + 1 - 2 * core)
    cands = [(d, lax.rem(c + j, m)) for j in range(1, m)]
    dps = [(lax.rem(d + j, n), c) for j in range(1, n)]
    greet(cands + dps)
    copies = []

    def send(*args):
        copies.append(push(*args))

    def arrived(ref, sem):
        pltpu.make_async_copy(ref, ref, sem).wait()

    for k in range(chunks):
        send(g_ref.at[k, :, 1 - core], r1.at[k], t1.at[k], v1.at[k], other)

    def stage_y(k):
        arrived(r1.at[k], v1.at[k])
        s1[k] = (g_ref[k, :, core].astype(F32) + r1[k].astype(F32)).astype(BF16)
        for j in range(1, duo):
            peer = lax.rem(y + j, duo)
            send(s1.at[k, peer], r2.at[k, j - 1], t2.at[k, j - 1], v2.at[k, j - 1], (d, 2 * peer + core))

    def stage_x(k):
        total = s1[k, y].astype(F32)
        for j in range(1, duo):
            arrived(r2.at[k, j - 1], v2.at[k, j - 1])
            total = total + r2[k, j - 1].astype(F32)
        s2[k] = total.astype(BF16)
        send(s2.at[k, :, 1 - x], r3.at[k], t3.at[k], v3.at[k], across)

    def stage_z(k):
        arrived(r3.at[k], v3.at[k])
        s3[k] = (s2[k, :, x].astype(F32) + r3[k].astype(F32)).astype(BF16)
        for j in range(1, half):
            peer = lax.rem(z + j, half)
            send(s3.at[k, peer], r4.at[k, j - 1], t4.at[k, j - 1], v4.at[k, j - 1], (2 * peer + x, c))

    def stage_cand(k):
        total = s3[k, z].astype(F32)
        for j in range(1, half):
            arrived(r4.at[k, j - 1], v4.at[k, j - 1])
            total = total + r4[k, j - 1].astype(F32)
        fin[k, c] = total.astype(BF16)
        for j in range(1, m):
            send(fin.at[k, c], fin.at[k, c], t5.at[k, j - 1], v5.at[k, j - 1], cands[j - 1])

    stages = (stage_x, stage_z, stage_cand)
    for k in range(chunks):
        stage_y(k)
    for t in range(chunks + 2):
        for lag, stage in enumerate(stages):
            if 0 <= t - lag < chunks:
                stage(t - lag)
    for k in range(chunks):
        for j in range(1, m):
            arrived(fin.at[k, lax.rem(c - j + m, m)], v5.at[k, j - 1])
    part = jnp.zeros((8, lanes), F32)
    for k in range(chunks):
        block = fin[k].astype(F32).reshape(m * rows // 8, 8, lanes)
        part = part + jnp.sum(block * block, axis=0)
    sq[...] = part
    r6[d] = part
    for j in range(1, n):
        send(sq, r6.at[d], t6.at[j - 1], v6.at[j - 1], dps[j - 1])
    for j in range(1, n):
        arrived(r6.at[lax.rem(d - j + n, n)], v6.at[j - 1])
    count = chunks * m * lanes * n * rows
    squares = jnp.sum(jnp.sum(jnp.sum(r6[...], axis=0), axis=0, keepdims=True), axis=1, keepdims=True)
    scale = 1.0 / (jnp.sqrt(squares / count) + EPS)
    for k in range(chunks):
        for i in range(m):
            at = (k * m + i) * lanes
            o_ref[:, at : at + lanes] = fin[k, i].astype(F32) * scale
    for copy in copies:
        copy.wait_send()


def reduce_update(grads, n, m):
    blocks, width, lanes = grads.shape
    rows = width // n
    duo, half = m // 2, n // 2
    chunks = blocks // m
    dma = pltpu.SemaphoreType.DMA
    vmem = pltpu.VMEM
    near, far = max(duo - 1, 1), max(half - 1, 1)
    return pl.pallas_call(
        functools.partial(reduce_kernel, n, m),
        in_specs=[pl.BlockSpec(memory_space=pltpu.VMEM)],
        out_specs=pl.BlockSpec(memory_space=pltpu.VMEM),
        out_shape=jax.ShapeDtypeStruct((rows, blocks * lanes), F32),
        scratch_shapes=[
            vmem((chunks, duo, half, 2, rows, lanes), BF16),
            vmem((chunks, duo, half, 2, rows, lanes), BF16),
            vmem((chunks, near, half, 2, rows, lanes), BF16),
            vmem((chunks, half, 2, rows, lanes), BF16),
            vmem((chunks, half, rows, lanes), BF16),
            vmem((chunks, half, rows, lanes), BF16),
            vmem((chunks, far, rows, lanes), BF16),
            vmem((chunks, m, rows, lanes), BF16),
            vmem((8, lanes), F32),
            vmem((n, 8, lanes), F32),
            dma((chunks,)), dma((chunks,)),
            dma((chunks, near)), dma((chunks, near)),
            dma((chunks,)), dma((chunks,)),
            dma((chunks, far)), dma((chunks, far)),
            dma((chunks, m - 1)), dma((chunks, m - 1)),
            dma((n - 1,)), dma((n - 1,)),
        ],
        compiler_params=pltpu.CompilerParams(
            collective_id=1, has_side_effects=True, vmem_limit_bytes=VMEM_LIMIT
        ),
        name="reduce_update",
    )(grads.reshape(chunks, duo, 2, half, 2, rows, lanes))


def shards(hidden, attn_weight, norm_gain, pos_bias, score_weight, pair_lengths, labels):
    q_local, c_local, seq, width = hidden.shape
    pairs = q_local * c_local
    heads = pos_bias.shape[0]
    head_size = width // heads
    n, m = lax.axis_size("dp"), lax.axis_size("cand")
    weights = gather_weights(attn_weight, n, m).reshape(4, m // 4, width, 4 * width // m)
    weights = weights.transpose(0, 2, 1, 3).reshape(4, width, width)
    pair_len = pair_lengths.reshape(pairs)
    len_col = pair_len.astype(F32).reshape(pairs, 1)
    gain = norm_gain.reshape(1, width)
    sw = score_weight.reshape(1, width)
    tokens = hidden.reshape(pairs, seq, width)
    normed_t, qk, probs, u, hsum = forward(tokens, pair_len, gain, weights, pos_bias)
    params = pltpu.CompilerParams(vmem_limit_bytes=VMEM_LIMIT)
    whole = lambda *shape: pl.BlockSpec(shape, lambda i: (0,) * len(shape))
    w_spec = pl.BlockSpec((2, width, width), lambda i: (1, 0, 0))
    col, wide = whole(pairs, 1), whole(pairs, width)
    ctx, pooled, score_col = pl.pallas_call(
        functools.partial(score_kernel, head_size),
        grid=(1,),
        in_specs=[whole(*u.shape), w_spec, wide, col, whole(1, width)],
        out_specs=[wide, wide, col],
        out_shape=[
            jax.ShapeDtypeStruct((pairs, width), BF16),
            jax.ShapeDtypeStruct((pairs, width), F32),
            jax.ShapeDtypeStruct((pairs, 1), F32),
        ],
        compiler_params=params,
        name="score_forward",
    )(u, weights, hsum.reshape(pairs, width), len_col, sw)
    scores = score_col.reshape(q_local, c_local)
    mine = jnp.stack([scores, labels.astype(F32)])
    every = lax.all_gather(mine, "cand", axis=2, tiled=True)
    all_scores, all_target = every[0], jnp.exp(every[1])
    highest = jnp.max(all_scores, axis=1)
    expsum = jnp.sum(jnp.exp(all_scores - highest[:, None]), axis=1)
    target_sum = jnp.sum(all_target, axis=1)
    target_dot = jnp.sum(all_target * all_scores, axis=1)
    loss = highest + jnp.log(expsum) - target_dot / target_sum
    target = jnp.exp(labels.astype(F32))
    score_grad = jnp.exp(scores - highest[:, None]) / expsum[:, None] - target / target_sum[:, None]
    duos, duo = heads // 2, 2 * head_size
    wc, grads = pl.pallas_call(
        functools.partial(middle_kernel, head_size),
        grid=(1,),
        in_specs=[col, wide, col, whole(1, width), whole(*u.shape), wide, w_spec],
        out_specs=[whole(*u.shape), pl.BlockSpec((2, duos, width, duo), lambda i: (1, 0, 0, 0))],
        out_shape=[
            jax.ShapeDtypeStruct(u.shape, BF16),
            jax.ShapeDtypeStruct((4, duos, width, duo), BF16),
        ],
        compiler_params=params,
        name="score_backward",
    )(score_grad.reshape(pairs, 1), pooled, len_col, sw, u, ctx, weights)
    grads = backward(normed_t, qk, probs, wc, grads)
    update = reduce_update(grads.reshape(4 * duos, width, duo), n, m)
    return (update, loss)


def solution(mesh):
    in_specs = (
        P("dp", "cand", None, None),
        P("dp", None),
        P(),
        P(),
        P(),
        P("dp", "cand"),
        P("dp", "cand"),
    )
    out_specs = (P("dp", None), P("dp"))
    return jax.shard_map(shards, mesh=mesh, in_specs=in_specs, out_specs=out_specs, check_vma=False)
```

```python
import functools

import jax
import jax.numpy as jnp
from jax import lax
from jax.experimental import pallas as pl
from jax.experimental.pallas import tpu as pltpu
from jax.sharding import PartitionSpec as P

EPS = 1e-06
F32 = jnp.float32
BF16 = jnp.bfloat16
VMEM_LIMIT = 60 * 1024 * 1024
NT = (((1,), (1,)), ((), ()))
TN = (((0,), (0,)), ((), ()))


def half_masks(lanes):
    lane = lax.broadcasted_iota(jnp.int32, (1, lanes), 1)
    low = (lane < lanes // 2).astype(F32)
    return low.astype(BF16), (1.0 - low).astype(BF16)


def stack_halves(block, low, high):
    return jnp.concatenate([block * low, block * high], axis=0)


def forward_kernel(hpad, len_ref, h_ref, gain_ref, w_ref, bias_ref, nt_ref, qk_ref, p_ref, u_ref, hsum_ref, norm_scr):
    batch, seq, width = h_ref.shape
    heads = bias_ref.shape[0]
    duo = 2 * (width // heads)
    step = pl.program_id(0)
    values = h_ref[...].reshape(batch * seq, width).astype(F32)
    factor = lax.rsqrt(jnp.mean(values * values, axis=-1, keepdims=True) + EPS)
    normed = (values * factor * gain_ref[...]).astype(BF16)
    norm_scr[...] = normed.reshape(batch, seq, width)
    nt_ref[...] = normed.T
    for part in range(2):
        proj = jnp.dot(normed, w_ref[part], preferred_element_type=F32)
        qk_ref[:, :, part * width : (part + 1) * width] = proj.astype(BF16).reshape(batch, seq, width)
    low, high = half_masks(duo)
    col = lax.broadcasted_iota(jnp.int32, (1, seq), 1)
    row = lax.broadcasted_iota(jnp.int32, (seq, 1), 0)

    def pair(i, carry):
        length = len_ref[step * batch + i]
        penalty = jnp.where(col < length, 0.0, 1.0) > 0.5
        live = row < length
        live2 = jnp.concatenate([live.astype(F32)] * 2, axis=0)
        sums = []
        for hp in range(heads // 2):
            q2 = qk_ref[i, :, hp * duo : (hp + 1) * duo]
            k2 = qk_ref[i, :, width + hp * duo : width + (hp + 1) * duo]
            logits = lax.dot_general(stack_halves(q2, low, high), k2, NT, preferred_element_type=F32)
            logits = logits + bias_ref[2 * hp : 2 * hp + 2].reshape(2 * seq, seq)
            logits = jnp.where(penalty, -1e30, logits)
            expo = jnp.exp(logits - jnp.max(logits, axis=-1, keepdims=True))
            inv = live2 / jnp.sum(expo, axis=-1, keepdims=True)
            probs = (expo * inv).astype(BF16)
            p_ref[i, 2 * hp : 2 * hp + 2] = probs.reshape(2, seq, seq)
            sums.append(jnp.sum(probs.astype(F32).reshape(2, seq, seq), axis=1))
        if hpad > heads:
            sums.append(jnp.zeros((hpad - heads, seq), F32))
        weights = jnp.concatenate(sums, axis=0).astype(BF16)
        u_ref[i] = jnp.dot(weights, norm_scr[i], preferred_element_type=F32).astype(BF16)
        rows = h_ref[i].astype(F32) * live.astype(F32)
        hsum_ref[i] = jnp.sum(rows, axis=0, keepdims=True)
        return carry

    lax.fori_loop(0, batch, pair, 0)


def forward(tokens, pair_len, gain, weights, pos_bias):
    pairs, seq, width = tokens.shape
    heads = pos_bias.shape[0]
    hpad = -(-heads // 16) * 16
    batch = 4 if pairs % 4 == 0 else 1
    full = lambda *shape: pl.BlockSpec(shape, lambda i: (0,) * len(shape))
    return pl.pallas_call(
        functools.partial(forward_kernel, hpad),
        grid=(pairs // batch,),
        in_specs=[
            pl.BlockSpec(memory_space=pltpu.SMEM),
            pl.BlockSpec((batch, seq, width), lambda i: (i, 0, 0)),
            full(1, width),
            full(2, width, width),
            full(heads, seq, seq),
        ],
        out_specs=[
            pl.BlockSpec((width, batch * seq), lambda i: (0, i)),
            pl.BlockSpec((batch, seq, 2 * width), lambda i: (i, 0, 0)),
            pl.BlockSpec((batch, heads, seq, seq), lambda i: (i, 0, 0, 0)),
            pl.BlockSpec((batch, hpad, width), lambda i: (i, 0, 0)),
            pl.BlockSpec((batch, 1, width), lambda i: (i, 0, 0)),
        ],
        out_shape=[
            jax.ShapeDtypeStruct((width, pairs * seq), BF16),
            jax.ShapeDtypeStruct((pairs, seq, 2 * width), BF16),
            jax.ShapeDtypeStruct((pairs, heads, seq, seq), BF16),
            jax.ShapeDtypeStruct((pairs, hpad, width), BF16),
            jax.ShapeDtypeStruct((pairs, 1, width), F32),
        ],
        scratch_shapes=[pltpu.VMEM((batch, seq, width), BF16)],
        compiler_params=pltpu.CompilerParams(vmem_limit_bytes=VMEM_LIMIT),
        cost_estimate=pl.CostEstimate(flops=30_000_000_000, bytes_accessed=24_000_000, transcendentals=0),
        name="attend_forward",
    )(pair_len, tokens, gain, weights, pos_bias)


def head_mask(hpad, width, head_size):
    lane = lax.broadcasted_iota(jnp.int32, (hpad, width), 1)
    head = lax.broadcasted_iota(jnp.int32, (hpad, width), 0)
    start = head * head_size
    return ((lane >= start) & (lane < start + head_size)).astype(F32)


def score_kernel(head_size, u_ref, w_ref, hsum_ref, len_ref, sw_ref, ctx_ref, pooled_ref, score_ref):
    pairs, hpad, width = u_ref.shape
    mixed = jnp.dot(u_ref[...].reshape(pairs * hpad, width), w_ref[0], preferred_element_type=F32)
    mask = head_mask(hpad, width, head_size)
    ctx = jnp.sum(mixed.reshape(pairs, hpad, width) * mask[None], axis=1)
    ctx_ref[...] = ctx.astype(BF16)
    share = 1.0 / len_ref[...]
    mean = ctx * share
    high = mean.astype(BF16)
    low = (mean - high.astype(F32)).astype(BF16)
    both = jnp.dot(jnp.concatenate([high, low], axis=0), w_ref[1], preferred_element_type=F32)
    pooled = hsum_ref[...] * share + both[:pairs] + both[pairs:]
    pooled_ref[...] = pooled
    factor = lax.rsqrt(jnp.mean(pooled * pooled, axis=-1, keepdims=True) + EPS)
    score_ref[...] = jnp.sum(pooled * factor * sw_ref[...], axis=-1, keepdims=True)


def middle_kernel(head_size, sg_ref, pooled_ref, len_ref, sw_ref, u_ref, ctx_ref, w_ref, wc_ref, gvo_ref):
    pairs, hpad, width = u_ref.shape
    pooled = pooled_ref[...]
    sw = sw_ref[...]
    factor = lax.rsqrt(jnp.mean(pooled * pooled, axis=-1, keepdims=True) + EPS)
    dot = jnp.sum(pooled * sw, axis=-1, keepdims=True) * (1.0 / width)
    grad = sg_ref[...] * (factor * sw - pooled * (factor * factor * factor * dot))
    out_grad = (grad / len_ref[...]).astype(BF16)
    cg = lax.dot_general(out_grad, w_ref[1], NT, preferred_element_type=F32).astype(BF16).astype(F32)
    mask = head_mask(hpad, width, head_size)
    spread = (cg[:, None, :] * mask[None]).astype(BF16).reshape(pairs * hpad, width)
    wc = lax.dot_general(spread, w_ref[0], NT, preferred_element_type=F32)
    wc_ref[...] = wc.astype(BF16).reshape(pairs, hpad, width)
    u = u_ref[...].reshape(pairs * hpad, width)
    _, duos, _, lanes = gvo_ref.shape
    gv = lax.dot_general(u, spread, TN, preferred_element_type=F32).astype(BF16)
    go = lax.dot_general(ctx_ref[...], out_grad, TN, preferred_element_type=F32).astype(BF16)
    for j in range(duos):
        gvo_ref[0, j] = gv[:, j * lanes : (j + 1) * lanes]
        gvo_ref[1, j] = go[:, j * lanes : (j + 1) * lanes]


MESH = pl.DeviceIdType.MESH


def greet(targets):
    barrier = pltpu.get_barrier_semaphore()
    for target in targets:
        pl.semaphore_signal(barrier, inc=1, device_id=target, device_id_type=MESH)
    pl.semaphore_wait(barrier, len(targets))


def push(src, dst, send, recv, target):
    copy = pltpu.make_async_remote_copy(
        src_ref=src, dst_ref=dst, send_sem=send, recv_sem=recv, device_id=target, device_id_type=MESH
    )
    copy.start()
    return copy


def gather_kernel(n, m, x_ref, o_ref, own_sem, z_send, x_send, y_send, c_send, recv):
    rows = x_ref.shape[0]
    wide = x_ref.shape[1] // m
    half, duo = n // 2, m // 2
    d, c = lax.axis_index("dp"), lax.axis_index("cand")
    z, x = d // 2, d % 2
    y, core = c // 2, c % 2
    across = (d + 1 - 2 * x, c)
    other = (d, c + 1 - 2 * core)
    zs = [(2 * lax.rem(z + j, half) + x, c) for j in range(1, half)]
    ys = [(d, 2 * lax.rem(y + j, duo) + core) for j in range(1, duo)]
    greet(zs + ys + [across, other])
    mine = x_ref.at[:, pl.ds(pl.multiple_of(c * wide, 128), wide)]
    copies = []
    for j in range(half - 1):
        copies.append(push(mine, o_ref.at[c, d], z_send.at[j], recv.at[c, d], zs[j]))
    copies.append(push(mine, o_ref.at[c, d], x_send.at[0], recv.at[c, d], across))
    local = []
    for k in range(m):
        local.append(
            pltpu.make_async_copy(x_ref.at[:, k * wide : (k + 1) * wide], o_ref.at[k, d], own_sem.at[k])
        )
        local[-1].start()

    def arrived(piece, block):
        ref = o_ref.at[piece, block]
        pltpu.make_async_copy(ref, ref, recv.at[piece, block]).wait()

    def spread(block, slot):
        ref = o_ref.at[c, block]
        for j in range(duo - 1):
            copies.append(push(ref, ref, y_send.at[slot, j], recv.at[c, block], ys[j]))
        copies.append(push(ref, ref, c_send.at[0, slot], recv.at[c, block], other))

    for j in range(1, half):
        block = 2 * lax.rem(z - j + half, half) + x
        arrived(c, block)
        ref = o_ref.at[c, block]
        copies.append(push(ref, ref, x_send.at[j], recv.at[c, block], across))
        spread(block, j - 1)
    far = []
    for j in range(half):
        block = 2 * lax.rem(z - j + half, half) + 1 - x
        arrived(c, block)
        spread(block, half - 1 + j)
    order = [2 * lax.rem(z - j + half, half) + x for j in range(1, half)]
    order += [2 * lax.rem(z - j + half, half) + 1 - x for j in range(half)]
    for slot, block in enumerate(order):
        for j in range(1, duo):
            piece = 2 * lax.rem(y - j + duo, duo) + core
            arrived(piece, block)
            ref = o_ref.at[piece, block]
            copies.append(push(ref, ref, c_send.at[j, slot], recv.at[piece, block], other))
    for slot, block in enumerate(order):
        for j in range(duo):
            arrived(2 * lax.rem(y - j + duo, duo) + 1 - core, block)
    for copy in local:
        copy.wait()
    for copy in copies:
        copy.wait_send()


def gather_weights(block, n, m):
    rows, total = block.shape
    dma = pltpu.SemaphoreType.DMA
    return pl.pallas_call(
        functools.partial(gather_kernel, n, m),
        in_specs=[pl.BlockSpec(memory_space=pltpu.VMEM)],
        out_specs=pl.BlockSpec(memory_space=pltpu.VMEM),
        out_shape=jax.ShapeDtypeStruct((m, n, rows, total // m), block.dtype),
        scratch_shapes=[
            dma((m,)), dma((n // 2,)), dma((n // 2,)), dma((n, max(m // 2 - 1, 1))), dma((m // 2, n)), dma((m, n))
        ],
        compiler_params=pltpu.CompilerParams(
            collective_id=0, has_side_effects=True, vmem_limit_bytes=VMEM_LIMIT
        ),
        name="gather_weights",
    )(block)


def stage_slots(duos, blocks, m):
    plan = []
    x_slot = -1
    for k in range(blocks // m):
        late = (k + 1) * m - 2 * duos
        first = 0 if late <= 0 else 3 * (-(-late // 2) - 1) + 2
        y_slot = first if first == 0 else first + 2
        x_slot = max(y_slot + 1, x_slot) + 3
        for stage, slot in enumerate((first, y_slot, x_slot, x_slot + 3, x_slot + 6)):
            plan.append((slot, stage, k))
    return sorted(plan)


def backward_kernel(n, m, nt_ref, q_ref, k_ref, p_ref, wc_ref, gvo_ref, o_ref, dp_scr, dqk_scr, grads,
                    r1, s1, r2, s2, r3, s3, r4, fin, sq, r6, own,
                    t1, v1, t2, v2, t3, v3, t4, v4, t5, v5, t6, v6):
    pairs, seq, span = q_ref.shape
    duos = dp_scr.shape[0]
    hp = pl.program_id(0)
    chunks, duo, half, _, rows, lanes = r1.shape
    d, c = lax.axis_index("dp"), lax.axis_index("cand")
    z, x = d // 2, d % 2
    y, core = c // 2, c % 2
    across = (d + 1 - 2 * x, c)
    other = (d, c + 1 - 2 * core)

    def arrived(ref, sem):
        pltpu.make_async_copy(ref, ref, sem).wait()

    def stage_core(k):
        push(grads.at[k * duo : (k + 1) * duo, 1 - core], r1.at[k], t1.at[k], v1.at[k], other)

    def stage_y(k):
        arrived(r1.at[k], v1.at[k])
        s1[k] = (grads[k * duo : (k + 1) * duo, core].astype(F32) + r1[k].astype(F32)).astype(BF16)
        for j in range(1, duo):
            peer = lax.rem(y + j, duo)
            push(s1.at[k, peer], r2.at[k, j - 1], t2.at[k, j - 1], v2.at[k, j - 1], (d, 2 * peer + core))

    def stage_x(k):
        total = s1[k, y].astype(F32)
        for j in range(1, duo):
            arrived(r2.at[k, j - 1], v2.at[k, j - 1])
            total = total + r2[k, j - 1].astype(F32)
        s2[k] = total.astype(BF16)
        push(s2.at[k, :, 1 - x], r3.at[k], t3.at[k], v3.at[k], across)

    def stage_z(k):
        arrived(r3.at[k], v3.at[k])
        s3[k] = (s2[k, :, x].astype(F32) + r3[k].astype(F32)).astype(BF16)
        for j in range(1, half):
            peer = lax.rem(z + j, half)
            push(s3.at[k, peer], r4.at[k, j - 1], t4.at[k, j - 1], v4.at[k, j - 1], (2 * peer + x, c))

    def stage_cand(k):
        total = s3[k, z].astype(F32)
        for j in range(1, half):
            arrived(r4.at[k, j - 1], v4.at[k, j - 1])
            total = total + r4[k, j - 1].astype(F32)
        fin[k, c] = total.astype(BF16)
        for j in range(1, m):
            target = (d, lax.rem(c + j, m))
            push(fin.at[k, c], fin.at[k, c], t5.at[k, j - 1], v5.at[k, j - 1], target)

    stages = (stage_core, stage_y, stage_x, stage_z, stage_cand)
    plan = stage_slots(duos, chunks * m, m)

    def run(place):
        for step in range(duos):
            items = [item for item in plan if item[0] == 3 * step + place]
            if items:

                @pl.when(hp == step)
                def _():
                    for _, stage, k in items:
                        stages[stage](k)

    @pl.when(hp == 0)
    def _():
        greet([(d, lax.rem(c + j, m)) for j in range(1, m)] + [(lax.rem(d + j, n), c) for j in range(1, n)])
        load = pltpu.make_async_copy(gvo_ref, grads.at[:duos], own)
        load.start()
        for i in range(pairs):
            part = jnp.dot(wc_ref[i], nt_ref[:, i * seq : (i + 1) * seq], preferred_element_type=F32)
            for j in range(duos):
                dp_scr[j, i] = part[2 * j : 2 * j + 2]
        load.wait()

    run(0)
    low, high = half_masks(span)

    def pair(i, carry):
        probs = p_ref[i].astype(F32)
        term = probs * dp_scr[hp, i][:, None, :]
        dlog = (term - probs * jnp.sum(term, axis=-1, keepdims=True)).astype(BF16)
        wide = jnp.concatenate([dlog[0], dlog[1]], axis=1)
        dq = jnp.dot(wide, stack_halves(k_ref[i], low, high), preferred_element_type=F32)
        dk = lax.dot_general(
            dlog.reshape(2 * seq, seq), stack_halves(q_ref[i], low, high), TN, preferred_element_type=F32
        )
        dqk_scr[i, :, :span] = dq.astype(BF16)
        dqk_scr[i, :, span:] = dk.astype(BF16)
        return carry

    lax.fori_loop(0, pairs, pair, 0, unroll=4)
    run(1)
    grad = jnp.dot(nt_ref[...], dqk_scr[...].reshape(pairs * seq, 2 * span), preferred_element_type=F32)
    grads[duos + hp, 0] = grad[:, :span].reshape(half, 2, rows, lanes).astype(BF16)
    grads[duos + hp, 1] = grad[:, span:].reshape(half, 2, rows, lanes).astype(BF16)
    run(2)

    @pl.when(hp == duos - 1)
    def _():
        for slot, stage, k in plan:
            if slot >= 3 * duos:
                stages[stage](k)
        for k in range(chunks):
            for j in range(1, m):
                arrived(fin.at[k, lax.rem(c - j + m, m)], v5.at[k, j - 1])
        part = jnp.zeros((8, lanes), F32)
        for k in range(chunks):
            block = fin[k].astype(F32).reshape(m * rows // 8, 8, lanes)
            part = part + jnp.sum(block * block, axis=0)
        sq[...] = part
        r6[d] = part
        for j in range(1, n):
            push(sq, r6.at[d], t6.at[j - 1], v6.at[j - 1], (lax.rem(d + j, n), c))
        for j in range(1, n):
            arrived(r6.at[lax.rem(d - j + n, n)], v6.at[j - 1])
        count = chunks * m * lanes * n * rows
        squares = jnp.sum(jnp.sum(jnp.sum(r6[...], axis=0), axis=0, keepdims=True), axis=1, keepdims=True)
        scale = 1.0 / (jnp.sqrt(squares / count) + EPS)
        for k in range(chunks):
            for i in range(m):
                at = k * m + i
                if at < 2 * duos:
                    at = 2 * duos + at
                else:
                    at = (at % 2) * duos + (at - 2 * duos) // 2
                o_ref[:, at * lanes : (at + 1) * lanes] = fin[k, i].astype(F32) * scale
        for k in range(chunks):
            arrived(r1.at[k], t1.at[k])
            arrived(r3.at[k], t3.at[k])
            for j in range(duo - 1):
                arrived(r2.at[k, j], t2.at[k, j])
            for j in range(half - 1):
                arrived(r4.at[k, j], t4.at[k, j])
            for j in range(m - 1):
                arrived(fin.at[k, c], t5.at[k, j])
        for j in range(n - 1):
            arrived(sq, t6.at[j])


def backward(normed_t, qk, probs, wc, gvo, n, m):
    pairs, heads, seq, _ = probs.shape
    width = normed_t.shape[0]
    lanes = 2 * (width // heads)
    duos = heads // 2
    rows, half, duo = width // n, n // 2, m // 2
    chunks = 4 * duos // m
    near, far = max(duo - 1, 1), max(half - 1, 1)
    dma = pltpu.SemaphoreType.DMA
    vmem = pltpu.VMEM
    return pl.pallas_call(
        functools.partial(backward_kernel, n, m),
        grid=(duos,),
        in_specs=[
            pl.BlockSpec((width, pairs * seq), lambda h: (0, 0)),
            pl.BlockSpec((pairs, seq, lanes), lambda h: (0, 0, h)),
            pl.BlockSpec((pairs, seq, lanes), lambda h: (0, 0, duos + h)),
            pl.BlockSpec((pairs, 2, seq, seq), lambda h: (0, h, 0, 0)),
            pl.BlockSpec(wc.shape, lambda h: (0, 0, 0)),
            pl.BlockSpec(memory_space=pl.ANY),
        ],
        out_specs=pl.BlockSpec((rows, 4 * width), lambda h: (0, 0)),
        out_shape=jax.ShapeDtypeStruct((rows, 4 * width), F32),
        scratch_shapes=[
            vmem((duos, pairs, 2, seq), F32),
            vmem((pairs, seq, 2 * lanes), BF16),
            vmem((2 * duos, 2, half, 2, rows, lanes), BF16),
            vmem((chunks, duo, half, 2, rows, lanes), BF16),
            vmem((chunks, duo, half, 2, rows, lanes), BF16),
            vmem((chunks, near, half, 2, rows, lanes), BF16),
            vmem((chunks, half, 2, rows, lanes), BF16),
            vmem((chunks, half, rows, lanes), BF16),
            vmem((chunks, half, rows, lanes), BF16),
            vmem((chunks, far, rows, lanes), BF16),
            vmem((chunks, m, rows, lanes), BF16),
            vmem((8, lanes), F32),
            vmem((n, 8, lanes), F32),
            pltpu.SemaphoreType.DMA,
            dma((chunks,)), dma((chunks,)),
            dma((chunks, near)), dma((chunks, near)),
            dma((chunks,)), dma((chunks,)),
            dma((chunks, far)), dma((chunks, far)),
            dma((chunks, m - 1)), dma((chunks, m - 1)),
            dma((n - 1,)), dma((n - 1,)),
        ],
        compiler_params=pltpu.CompilerParams(
            collective_id=1, has_side_effects=True, vmem_limit_bytes=VMEM_LIMIT
        ),
        cost_estimate=pl.CostEstimate(flops=30_000_000_000, bytes_accessed=20_000_000, transcendentals=0),
        name="backward_reduce",
    )(normed_t, qk, qk, probs, wc, gvo.reshape(duos, 2, half, 2, rows, lanes))


def shards(hidden, attn_weight, norm_gain, pos_bias, score_weight, pair_lengths, labels):
    q_local, c_local, seq, width = hidden.shape
    pairs = q_local * c_local
    heads = pos_bias.shape[0]
    head_size = width // heads
    n, m = lax.axis_size("dp"), lax.axis_size("cand")
    weights = gather_weights(attn_weight, n, m).reshape(4, m // 4, width, 4 * width // m)
    weights = weights.transpose(0, 2, 1, 3).reshape(4, width, width)
    pair_len = pair_lengths.reshape(pairs)
    len_col = pair_len.astype(F32).reshape(pairs, 1)
    gain = norm_gain.reshape(1, width)
    sw = score_weight.reshape(1, width)
    tokens = hidden.reshape(pairs, seq, width)
    normed_t, qk, probs, u, hsum = forward(tokens, pair_len, gain, weights, pos_bias)
    params = pltpu.CompilerParams(vmem_limit_bytes=VMEM_LIMIT)
    whole = lambda *shape: pl.BlockSpec(shape, lambda i: (0,) * len(shape))
    w_spec = pl.BlockSpec((2, width, width), lambda i: (1, 0, 0))
    col, wide = whole(pairs, 1), whole(pairs, width)
    ctx, pooled, score_col = pl.pallas_call(
        functools.partial(score_kernel, head_size),
        grid=(1,),
        in_specs=[whole(*u.shape), w_spec, wide, col, whole(1, width)],
        out_specs=[wide, wide, col],
        out_shape=[
            jax.ShapeDtypeStruct((pairs, width), BF16),
            jax.ShapeDtypeStruct((pairs, width), F32),
            jax.ShapeDtypeStruct((pairs, 1), F32),
        ],
        compiler_params=params,
        name="score_forward",
    )(u, weights, hsum.reshape(pairs, width), len_col, sw)
    scores = score_col.reshape(q_local, c_local)
    mine = jnp.stack([scores, labels.astype(F32)])
    every = lax.all_gather(mine, "cand", axis=2, tiled=True)
    all_scores, all_target = every[0], jnp.exp(every[1])
    highest = jnp.max(all_scores, axis=1)
    expsum = jnp.sum(jnp.exp(all_scores - highest[:, None]), axis=1)
    target_sum = jnp.sum(all_target, axis=1)
    target_dot = jnp.sum(all_target * all_scores, axis=1)
    loss = highest + jnp.log(expsum) - target_dot / target_sum
    target = jnp.exp(labels.astype(F32))
    score_grad = jnp.exp(scores - highest[:, None]) / expsum[:, None] - target / target_sum[:, None]
    duos, duo = heads // 2, 2 * head_size
    wc, gvo = pl.pallas_call(
        functools.partial(middle_kernel, head_size),
        grid=(1,),
        in_specs=[col, wide, col, whole(1, width), whole(*u.shape), wide, w_spec],
        out_specs=[whole(*u.shape), whole(2, duos, width, duo)],
        out_shape=[
            jax.ShapeDtypeStruct(u.shape, BF16),
            jax.ShapeDtypeStruct((2, duos, width, duo), BF16),
        ],
        compiler_params=params,
        name="score_backward",
    )(score_grad.reshape(pairs, 1), pooled, len_col, sw, u, ctx, weights)
    update = backward(normed_t, qk, probs, wc, gvo, n, m)
    return (update, loss)


def solution(mesh):
    in_specs = (
        P("dp", "cand", None, None),
        P("dp", None),
        P(),
        P(),
        P(),
        P("dp", "cand"),
        P("dp", "cand"),
    )
    out_specs = (P("dp", None), P("dp"))
    return jax.shard_map(shards, mesh=mesh, in_specs=in_specs, out_specs=out_specs, check_vma=False)
```
